32 devices in a mesh: pool: 2 (over core), seq: 4 (over y, x), head: 4 (over z).
Axes of the slice: x: 2, y: 2, z: 4, core: 2. Of those that a mesh axis runs over, the one named last changes fastest.
Arguments:
- x_in: bfloat16 [1, 4096, 8, 2048], P(None, 'seq', 'head', 'pool'), may hold values from -6 to 6
- gate_in: bfloat16 [1, 4096, 8, 2048], P(None, 'seq', 'head', 'pool'), may hold values from -6 to 6
- dt_raw: bfloat16 [1, 4096, 8, 32], P(None, 'seq', 'head', 'pool'), may hold values from -4 to 4
- b_in: bfloat16 [1, 4096, 8, 256], P(None, 'seq', 'head'), may hold values from -0.375 to 0.375
- c_in: bfloat16 [1, 4096, 8, 256], P(None, 'seq', 'head'), may hold values from -6 to 6
- lengths: int32 [1], replicated, may hold values from 1024 to 4096
- decay_rate: float32 [8, 32], P('head', 'pool'), may hold values from 0.0001 to 0.05
- skip_gain: float32 [8, 32], P('head', 'pool'), may hold values from 0.5 to 2
- norm_gain: float32 [8, 2048], P('head', 'pool'), may hold values from 0.5 to 1.5
- dec_states: float32 [16, 8, 32, 64, 256], P('seq', 'head', 'pool'), may hold values from -18 to 18
- dec_x: bfloat16 [8, 16, 8, 2048], P(None, 'seq', 'head', 'pool'), may hold values from -6 to 6
- dec_gate: bfloat16 [8, 16, 8, 2048], P(None, 'seq', 'head', 'pool'), may hold values from -6 to 6
- dec_dt: bfloat16 [8, 16, 8, 32], P(None, 'seq', 'head', 'pool'), may hold values from -4 to 4
- dec_b: bfloat16 [8, 16, 8, 256], P(None, 'seq', 'head'), may hold values from -0.375 to 0.375
- dec_c: bfloat16 [8, 16, 8, 256], P(None, 'seq', 'head'), may hold values from -6 to 6
- slots: int32 [16], P('seq'), may hold values from -1 to 0, as said below
Outputs:
- prefill_out: bfloat16 [1, 4096, 8, 2048], P(None, 'seq', 'head', 'pool')
- decode_out: bfloat16 [8, 16, 8, 2048], P(None, 'seq', 'head', 'pool')
The draws below stay inside these ranges and needn't reach their ends.
Inputs may be any that keep to these rules, and one draw needn't show every extreme that they name: `lengths`: valid positions of each prompt; later positions are padding. `slots`: each aligned block of 4 decode sequences holds at least one that continues a prompt and at least one that keeps its own state.
All inputs are finite; a program needn't handle non-finite values.
Results may differ from the reference program's by a relative error of at most 0.001.
Values sent between devices are 32-bit elements; how exact they have to be, the bound alone decides.
A program may use at most 128 MiB of HBM per device.

```python
import math
import jax
import jax.numpy as jnp
from jax import lax

HEADS = 256
HEAD_DIM = 64
STATE = 256
GROUPS = 8
PROMPTS = 1
SPAN = 256
DEC_DEV = 4
STEPS = 8
LENGTH = 4096
DECODES = 16


def draw_slots(key, part):
    first_key, second_key, third_key = jax.random.split(jax.random.fold_in(key, 11), 3)
    block_count = DECODES // DEC_DEV
    base = jax.random.randint(first_key, (DECODES,), -1, PROMPTS)
    offset = jax.random.randint(second_key, (block_count,), 0, DEC_DEV)
    chosen = jax.random.randint(third_key, (block_count,), 0, PROMPTS)
    rows = jnp.arange(DECODES, dtype=jnp.int32)
    block_of = rows // DEC_DEV
    inside = rows % DEC_DEV
    place = offset[block_of]
    result = jnp.where(inside == place, chosen[block_of], jnp.where(inside == (place + 1) % DEC_DEV, -1, base))
    return result.astype(jnp.int32)


def level_of(stream_key, extent, cuts, smallest, top_value):
    def one(position, blocks):
        steps = jax.random.uniform(jax.random.fold_in(jax.random.fold_in(stream_key, 6), position), (blocks,), jnp.float32, smallest / len(cuts), top_value / len(cuts))
        return jnp.repeat(jnp.exp(steps), extent[position] // blocks).reshape((-1,) + (1,) * (len(extent) - position - 1))

    level = one(*cuts[0])
    for cut in cuts[1:]:
        level = level * one(*cut)
    return level


def centred(key, dims, spread, limit, pieces=(), kind=jnp.bfloat16):
    values = spread * jax.random.normal(key, dims, jnp.float32)
    if pieces:
        values = values * level_of(key, dims, pieces, -0.22, 0.18)
    return jnp.clip(values, -limit, limit).astype(kind)


def setup_inputs(seed: int = 0) -> dict:
    arg_keys = jax.random.split(jax.random.key(seed), 17)
    return {
        "x_in": centred(arg_keys[0], (PROMPTS, LENGTH, GROUPS, HEADS // GROUPS * HEAD_DIM), 1.0, 6.0, ((1, 4), (2, 4), (3, 2))),
        "gate_in": centred(arg_keys[1], (PROMPTS, LENGTH, GROUPS, HEADS // GROUPS * HEAD_DIM), 1.0, 6.0, ((1, 4), (2, 4), (3, 2))),
        "dt_raw": centred(arg_keys[2], (PROMPTS, LENGTH, GROUPS, HEADS // GROUPS), 1.0, 4.0, ((1, 4), (2, 4), (3, 2))),
        "b_in": centred(arg_keys[3], (PROMPTS, LENGTH, GROUPS, STATE), STATE ** -0.5, 0.375, ((1, 4), (2, 4))),
        "c_in": centred(arg_keys[4], (PROMPTS, LENGTH, GROUPS, STATE), 1.0, 6.0, ((1, 4), (2, 4))),
        "lengths": jax.random.randint(arg_keys[5], (PROMPTS,), LENGTH // 4, LENGTH + 1).astype(jnp.int32),
        "decay_rate": jnp.clip(jnp.exp(math.log(0.05) - 6.214608 * jax.random.uniform(arg_keys[6], (GROUPS, HEADS // GROUPS), jnp.float32) ** level_of(arg_keys[6], (GROUPS, HEADS // GROUPS), ((0, 4), (1, 2)), -0.2, 0.2)), 0.0001, 0.05),
        "skip_gain": jnp.clip(0.5 + 1.5 * jax.random.uniform(arg_keys[7], (GROUPS, HEADS // GROUPS), jnp.float32) ** level_of(arg_keys[7], (GROUPS, HEADS // GROUPS), ((0, 4), (1, 2)), -0.2, 0.2), 0.5, 2.0),
        "norm_gain": jnp.clip(1.0 + 0.1 * jax.random.normal(arg_keys[8], (GROUPS, HEADS // GROUPS * HEAD_DIM), jnp.float32), 0.5, 1.5),
        "dec_states": centred(arg_keys[9], (DECODES, GROUPS, HEADS // GROUPS, HEAD_DIM, STATE), 3.0, 18.0, ((0, 4), (1, 4), (2, 2)), jnp.float32),
        "dec_x": centred(arg_keys[10], (STEPS, DECODES, GROUPS, HEADS // GROUPS * HEAD_DIM), 1.0, 6.0, ((1, 4), (2, 4), (3, 2))),
        "dec_gate": centred(arg_keys[11], (STEPS, DECODES, GROUPS, HEADS // GROUPS * HEAD_DIM), 1.0, 6.0, ((1, 4), (2, 4), (3, 2))),
        "dec_dt": centred(arg_keys[12], (STEPS, DECODES, GROUPS, HEADS // GROUPS), 1.0, 4.0, ((1, 4), (2, 4), (3, 2))),
        "dec_b": centred(arg_keys[13], (STEPS, DECODES, GROUPS, STATE), STATE ** -0.5, 0.375, ((1, 4), (2, 4))),
        "dec_c": centred(arg_keys[14], (STEPS, DECODES, GROUPS, STATE), 1.0, 6.0, ((1, 4), (2, 4))),
        "slots": draw_slots(jax.random.fold_in(arg_keys[16], 71), 0),
    }


highest = lax.Precision.HIGHEST
epsilon = 1e-05

def gated_norm(values, gate_part, gain_part):
    mixed = values * jax.nn.silu(gate_part.astype(jnp.float32))
    power = lax.optimization_barrier(jnp.mean(mixed * mixed, axis=-1, keepdims=True))
    return mixed * lax.rsqrt(power + epsilon) * gain_part

def reference(x_in, gate_in, dt_raw, b_in, c_in, lengths, decay_rate, skip_gain, norm_gain, dec_states, dec_x, dec_gate, dec_dt, dec_b, dec_c, slots):
    per_group = HEADS // GROUPS
    spans = LENGTH // SPAN
    live_mask = (jnp.arange(LENGTH, dtype=jnp.int32)[None, :] < lengths[:, None]).astype(jnp.float32)
    step_size = jax.nn.softplus(dt_raw.astype(jnp.float32)) * live_mask[:, :, None, None]
    log_decay = -step_size * decay_rate
    values = x_in.astype(jnp.float32).reshape(PROMPTS, LENGTH, GROUPS, per_group, HEAD_DIM)
    inflow = values * step_size[..., None]

    def blocks(array):
        return jnp.swapaxes(array.reshape((PROMPTS, spans, SPAN) + array.shape[2:]), 0, 1)
    positions = jnp.arange(SPAN)
    lower_mask = positions[:, None] >= positions[None, :]

    def span_step(running, inputs):
        flow, vals, b_part, c_part, logs, alive = inputs
        cumulative = jnp.moveaxis(jnp.cumsum(logs, axis=1), 1, -1)
        scores = jnp.einsum('bign,bjgn->bgij', c_part, b_part, precision=highest)
        gaps = cumulative[..., :, None] - cumulative[..., None, :]
        weights = jnp.exp(jnp.where(lower_mask, gaps, -jnp.inf)) * scores[:, :, None]
        inner = jnp.einsum('bghij,bjghp->bighp', weights, flow, precision=highest)
        outer = jnp.einsum('bign,bghpn->bghip', c_part, running, precision=highest) * jnp.exp(cumulative)[..., None]
        outer = jnp.transpose(outer, (0, 3, 1, 2, 4))
        output = (inner + outer + skip_gain[:, :, None] * vals) * alive[:, :, None, None, None]
        last = cumulative[..., -1:]
        carried = jnp.einsum('bjghp,bjgn,bghj->bghpn', flow, b_part, jnp.exp(last - cumulative), precision=highest)
        running = running * jnp.exp(last)[..., None] + carried
        return (running, output)
    initial = jnp.zeros((PROMPTS, GROUPS, per_group, HEAD_DIM, STATE), jnp.float32)
    final, outputs = lax.scan(span_step, initial, (blocks(inflow), blocks(values), blocks(b_in.astype(jnp.float32)), blocks(c_in.astype(jnp.float32)), blocks(log_decay), blocks(live_mask)))
    outputs = jnp.swapaxes(outputs, 0, 1).reshape(PROMPTS, LENGTH, GROUPS, per_group * HEAD_DIM)
    prefill_out = gated_norm(outputs, gate_in, norm_gain).astype(jnp.bfloat16)
    inserted = final[jnp.maximum(slots, 0).astype(jnp.int32)]
    start = jnp.where((slots >= 0)[:, None, None, None, None], inserted, dec_states)

    def decode_step(states, inputs):
        x_step, gate_step, dt_step, b_step, c_step = inputs
        step_dt = jax.nn.softplus(dt_step.astype(jnp.float32))
        vals = x_step.astype(jnp.float32).reshape(DECODES, GROUPS, per_group, HEAD_DIM)
        keep = jnp.exp(-step_dt * decay_rate)
        flow = vals * step_dt[..., None]
        states = states * keep[..., None, None] + flow[..., None] * b_step.astype(jnp.float32)[:, :, None, None, :]
        result = jnp.einsum('dgn,dghpn->dghp', c_step.astype(jnp.float32), states, precision=highest) + skip_gain[..., None] * vals
        normed = gated_norm(result.reshape(DECODES, GROUPS, per_group * HEAD_DIM), gate_step, norm_gain)
        return (states, normed.astype(jnp.bfloat16))
    end_states, decode_out = lax.scan(decode_step, start, (dec_x, dec_gate, dec_dt, dec_b, dec_c))
    return (prefill_out, decode_out)
```

```python
import jax
import jax.numpy as jnp
from jax import lax
from jax.experimental import pallas as pl
from jax.experimental.pallas import tpu as pltpu
from jax.sharding import PartitionSpec as P

HEADS = 256
HEAD_DIM = 64
GROUPS = 8
SPAN = 256

highest = lax.Precision.HIGHEST
epsilon = 1e-05
F32 = jnp.float32
BF16 = jnp.bfloat16


def split(a):
    hi = a.astype(BF16)
    lo = (a - hi.astype(F32)).astype(BF16)
    return hi, lo


def mm(a, b, dims=((1,), (0,))):
    return lax.dot_general(a, b, (dims, ((), ())), preferred_element_type=F32)


def expander(heads, width):
    head_of = lax.broadcasted_iota(jnp.int32, (heads, width), 1) // (width // heads)
    return (head_of == lax.broadcasted_iota(jnp.int32, (heads, width), 0)).astype(BF16)


def expand(a, spread):
    hi, lo = split(a)
    return mm(hi, spread) + mm(lo, spread)


def cumulative_logs(step, rate):
    span = step.shape[0]
    lower = (
        lax.broadcasted_iota(jnp.int32, (span, span), 0)
        >= lax.broadcasted_iota(jnp.int32, (span, span), 1)
    ).astype(BF16)
    logs = -step * rate
    hi = logs.astype(BF16)
    rest = logs - hi.astype(F32)
    mid, lo = split(rest)
    return mm(lower, hi) + (mm(lower, mid) + mm(lower, lo))


def state_kernel(x_ref, b_ref, step_ref, rate_ref, *refs):
    out_refs, run_ref = refs[:-1], refs[-1]
    width = x_ref.shape[1]
    heads = step_ref.shape[1]
    spread = expander(heads, width)

    @pl.when(pl.program_id(0) == 0)
    def _():
        run_ref[...] = jnp.zeros_like(run_ref)

    step = step_ref[...]
    cum = cumulative_logs(step, rate_ref[...])
    flow = x_ref[...].astype(F32) * expand(step * jnp.exp(-cum), spread)
    flow_hi, flow_lo = split(flow)
    b = b_ref[...]
    dims = ((0,), (0,))
    added = mm(b, flow_hi, dims) + mm(b, flow_lo, dims)
    kept = expand(jnp.exp(cum[-8:]), spread)[7:8]
    run_ref[...] = (run_ref[...] + added) * kept

    @pl.when(pl.program_id(0) == pl.num_programs(0) - 1)
    def _():
        part = width // len(out_refs)
        for i, out_ref in enumerate(out_refs):
            out_ref[...] = run_ref[:, i * part : (i + 1) * part]


def inner_kernel(x_ref, b_ref, c_ref, step_ref, rate_ref, skip_ref, y_ref, entry_ref, run_ref, log_ref):
    span, width = x_ref.shape
    heads = step_ref.shape[1]
    spread = expander(heads, width)

    @pl.when(pl.program_id(1) == 0)
    def _():
        run_ref[...] = jnp.zeros_like(run_ref)
        log_ref[...] = jnp.zeros_like(log_ref)

    step = step_ref[...]
    cum = cumulative_logs(step, rate_ref[...])
    values = x_ref[...].astype(F32)
    flow_hi, flow_lo = split(values * expand(step * jnp.exp(-cum), spread))
    b = b_ref[...]
    c = c_ref[...]
    scores = mm(c, b, ((1,), (1,)))
    row = lax.broadcasted_iota(jnp.int32, (span, span), 0)
    col = lax.broadcasted_iota(jnp.int32, (span, span), 1)
    score_hi, score_lo = split(jnp.where(row >= col, scores, 0.0))
    run_hi, run_lo = split(run_ref[...])
    total = mm(score_hi, flow_hi) + mm(score_lo, flow_hi) + mm(score_hi, flow_lo)
    total = total + mm(c, run_hi) + mm(c, run_lo)
    y_ref[...] = total * expand(jnp.exp(cum), spread) + values * skip_ref[...]
    entry_ref[...] = jnp.exp(cum + log_ref[0:1])
    log_ref[...] = log_ref[...] + cum[span - 1 : span]
    dims = ((0,), (0,))
    added = mm(b, flow_hi, dims) + mm(b, flow_lo, dims)
    kept = expand(jnp.exp(cum[-8:]), spread)[7:8]
    run_ref[...] = (run_ref[...] + added) * kept


def mix_kernel(y_ref, c_ref, entry_ref, incoming_ref, gate_ref, live_ref, mixed_ref, power_ref):
    width = y_ref.shape[1]
    heads = entry_ref.shape[1]
    spread = expander(heads, width)
    inc_hi, inc_lo = split(incoming_ref[...])
    c = c_ref[...]
    extra = mm(c, inc_hi) + mm(c, inc_lo)
    y = y_ref[...] + extra * expand(entry_ref[...], spread)
    gate = gate_ref[...].astype(F32)
    mixed = y * (gate / (1.0 + jnp.exp(-gate))) * live_ref[...]
    mixed_ref[...] = mixed
    power_ref[...] = jnp.sum(mixed * mixed, axis=1, keepdims=True)


def decode_kernel(state_ref, c_ref, out_ref):
    hi, lo = split(state_ref[...])
    c = c_ref[...]
    dims = ((1,), (1,))
    out_ref[...] = mm(c, hi, dims) + mm(c, lo, dims)


def params(*kinds):
    return pltpu.CompilerParams(
        dimension_semantics=kinds, vmem_limit_bytes=56 * 1024 * 1024
    )


def shards(
    x_in, gate_in, dt_raw, b_in, c_in, lengths, decay_rate, skip_gain, norm_gain,
    dec_states, dec_x, dec_gate, dec_dt, dec_b, dec_c, slots,
):
    prompts, length_dev, groups, width = x_in.shape
    heads = dt_raw.shape[3]
    head_dim = width // heads
    state_size = b_in.shape[3]
    count = lax.axis_size("seq")
    own = lax.axis_index("seq")
    full_width = HEADS // GROUPS * HEAD_DIM
    span = SPAN
    spans = length_dev // span
    steps, dec_rows = dec_x.shape[:2]

    where_now = own * length_dev + jnp.arange(length_dev, dtype=jnp.int32)
    live = (where_now < lengths[0]).astype(F32)

    def grouped(a):
        return jnp.swapaxes(a[0], 0, 1)

    x = grouped(x_in)
    b = grouped(b_in)
    step = jax.nn.softplus(grouped(dt_raw).astype(F32)) * live[None, :, None]
    rates = decay_rate[:, None, :]
    own_logs = -jnp.sum(step, axis=1) * decay_rate

    log_rows = jnp.pad(
        jnp.repeat(own_logs, head_dim, axis=1).reshape(-1, state_size), ((0, -groups * width // state_size % 8), (0, 0))
    )
    c_count = steps * dec_rows * groups
    packed = jnp.concatenate([dec_c.astype(F32).reshape(-1, state_size), log_rows])
    packed = lax.all_gather(packed, "seq")
    all_logs = packed[:, c_count:].reshape(count, -1)[:, : groups * width].reshape(count, groups, width)
    all_c = packed[:, :c_count].reshape(count, steps, dec_rows, groups, state_size)

    pieces = 2
    part = width // pieces
    locals_ = []
    for g in range(groups):
        locals_.append(
            pl.pallas_call(
                state_kernel,
                grid=(spans,),
                in_specs=[
                    pl.BlockSpec((None, span, width), lambda i, g=g: (g, i, 0)),
                    pl.BlockSpec((None, span, state_size), lambda i, g=g: (g, i, 0)),
                    pl.BlockSpec((None, span, heads), lambda i, g=g: (g, i, 0)),
                    pl.BlockSpec((None, 1, heads), lambda i, g=g: (g, 0, 0)),
                ],
                out_specs=[pl.BlockSpec((state_size, part), lambda i: (0, 0))] * pieces,
                out_shape=[jax.ShapeDtypeStruct((state_size, part), F32)] * pieces,
                scratch_shapes=[pltpu.VMEM((state_size, width), F32)],
                compiler_params=params("arbitrary"),
                name=f"local_state_{g}",
            )(x, b, step, rates)
        )

    places = jnp.arange(count)

    def block_decay(low, high):
        inside = (places >= low) & (places < high)
        return jnp.exp(jnp.sum(jnp.where(inside[:, None, None], all_logs, 0.0), axis=0))

    def row_of(a, g, i):
        return a[g][None, i * part : (i + 1) * part]

    rounds = []
    bit = 1
    while bit < count:
        pairs = [
            (i, i ^ bit)
            for i in range(count)
            if not i & bit or (i | (2 * bit - 1)) != count - 1
        ]
        base = own - own % bit
        other = base ^ bit
        rounds.append(
            (bit, pairs, block_decay(base, own), block_decay(base, base + bit), block_decay(other, other + bit))
        )
        bit *= 2
    incoming = []
    for g in range(groups):
        done = []
        for i in range(pieces):
            total = locals_[g][i]
            prefix = jnp.zeros_like(total)
            for bit, pairs, before, mine, others in rounds:
                got = lax.ppermute(total, "seq", pairs)
                upper = (own & bit) != 0
                prefix = jnp.where(upper, row_of(before, g, i) * got + prefix, prefix)
                if 2 * bit < count:
                    total = jnp.where(
                        upper,
                        row_of(mine, g, i) * got + total,
                        row_of(others, g, i) * total + got,
                    )
            done.append(prefix)
        incoming.append(jnp.concatenate(done, axis=1))
    incoming = jnp.stack(incoming)

    later = block_decay(own + 1, count)
    shares = []
    for g in range(groups):
        cs = all_c[:, :, :, g].reshape(-1, state_size)
        local = jnp.concatenate(locals_[g], axis=1)
        shares.append(jnp.dot(cs, local, precision=highest) * later[g][None])
    shares = jnp.stack(shares).reshape(groups, count, steps * dec_rows, width)
    carried = lax.dynamic_index_in_dim(shares, own, 1, False)
    for hop in range(1, count):
        target = (own + hop) % count
        carried = carried + lax.ppermute(
            lax.dynamic_index_in_dim(shares, target, 1, False),
            "seq",
            [(i, (i + hop) % count) for i in range(count)],
        )
    carried = jnp.transpose(carried.reshape(groups, steps, dec_rows, width), (1, 2, 0, 3))

    gate = grouped(gate_in)
    c = grouped(c_in)
    skip_row = jnp.repeat(skip_gain, head_dim, axis=1)

    def of_span(last):
        return pl.BlockSpec((None, span, last), lambda g, i: (g, i, 0))

    def of_group(rows, last):
        return pl.BlockSpec((None, rows, last), lambda g, i: (g, 0, 0))

    y, entry = pl.pallas_call(
        inner_kernel,
        grid=(groups, spans),
        in_specs=[
            of_span(width), of_span(state_size), of_span(state_size), of_span(heads),
            of_group(1, heads), of_group(1, width),
        ],
        out_specs=[of_span(width), of_span(heads)],
        out_shape=[
            jax.ShapeDtypeStruct((groups, length_dev, width), F32),
            jax.ShapeDtypeStruct((groups, length_dev, heads), F32),
        ],
        scratch_shapes=[pltpu.VMEM((state_size, width), F32), pltpu.VMEM((8, heads), F32)],
        compiler_params=params("arbitrary", "arbitrary"),
        name="inner",
    )(x, b, c, step, rates, skip_row[:, None])

    dec_c_rows = jnp.transpose(dec_c, (1, 2, 0, 3))
    kept = pl.pallas_call(
        decode_kernel,
        grid=(dec_rows, groups),
        in_specs=[
            pl.BlockSpec((None, None, width, state_size), lambda d, g: (d, g, 0, 0)),
            pl.BlockSpec((None, None, steps, state_size), lambda d, g: (d, g, 0, 0)),
        ],
        out_specs=pl.BlockSpec((None, None, steps, width), lambda d, g: (d, g, 0, 0)),
        out_shape=jax.ShapeDtypeStruct((dec_rows, groups, steps, width), F32),
        compiler_params=params("arbitrary", "arbitrary"),
        name="decode_products",
    )(dec_states.reshape(dec_rows, groups, width, state_size), dec_c_rows)
    kept = jnp.transpose(kept, (2, 0, 1, 3))
    from_start = jnp.where((slots >= 0)[None, :, None, None], carried, kept)
    sdt = jax.nn.softplus(dec_dt.astype(F32))
    cum = jnp.cumsum(-sdt * decay_rate, axis=0)
    products = jnp.einsum(
        "sdgn,rdgn->srdg", dec_c.astype(F32), dec_b.astype(F32), precision=highest
    )
    order = jnp.arange(steps)
    allowed = (order[:, None] >= order[None, :])[:, :, None, None, None]
    weights = jnp.exp(jnp.where(allowed, cum[:, None] - cum[None], -jnp.inf))
    weights = weights * products[..., None] * sdt[None]
    dec_vals = dec_x.astype(F32).reshape(steps, dec_rows, groups, heads, head_dim)
    result = jnp.sum(weights[..., None] * dec_vals[None], axis=1)
    result = result + skip_gain[..., None] * dec_vals
    result = result.reshape(dec_x.shape) + from_start * jnp.repeat(
        jnp.exp(cum), head_dim, axis=3
    )
    gated = result * jax.nn.silu(dec_gate.astype(F32))
    dec_power = jnp.sum(gated * gated, axis=-1)

    mixed, power = pl.pallas_call(
        mix_kernel,
        grid=(groups, spans),
        in_specs=[
            of_span(width), of_span(state_size), of_span(heads), of_group(state_size, width),
            of_span(width), pl.BlockSpec((span, 1), lambda g, i: (i, 0)),
        ],
        out_specs=[of_span(width), of_span(1)],
        out_shape=[
            jax.ShapeDtypeStruct((groups, length_dev, width), F32),
            jax.ShapeDtypeStruct((groups, length_dev, 1), F32),
        ],
        compiler_params=params("arbitrary", "arbitrary"),
        name="mix",
    )(y, c, entry, incoming, gate, live[:, None])

    pool = lax.axis_size("pool")
    powers = jnp.concatenate([power.reshape(-1), dec_power.reshape(-1)])
    both = powers
    for hop in range(1, pool):
        both = both + lax.ppermute(powers, "pool", [(i, (i + hop) % pool) for i in range(pool)])
    both = lax.rsqrt(both / full_width + epsilon)
    scale = both[: power.size].reshape(power.shape)
    dec_scale = both[power.size :].reshape(dec_power.shape)
    prefill_out = (mixed * scale * norm_gain[:, None]).astype(BF16)
    prefill_out = jnp.swapaxes(prefill_out, 0, 1)[None]
    decode_out = (gated * dec_scale[..., None] * norm_gain).astype(BF16)
    return (prefill_out, decode_out)


def solution(mesh):
    wide = P(None, "seq", "head", "pool")
    shared = P(None, "seq", "head", None)
    per_head = P("head", "pool")
    in_specs = (
        wide, wide, wide, shared, shared, P(), per_head, per_head, per_head,
        P("seq", "head", "pool", None, None), wide, wide, wide, shared, shared, P("seq"),
    )
    return jax.shard_map(
        shards, mesh=mesh, in_specs=in_specs, out_specs=(wide, wide), check_vma=False
    )
```

```python
import jax
import jax.numpy as jnp
from functools import partial
from jax import lax
from jax.experimental import pallas as pl
from jax.experimental.pallas import tpu as pltpu
from jax.sharding import PartitionSpec as P

HEADS = 256
HEAD_DIM = 64
GROUPS = 8
SPAN = 256

highest = lax.Precision.HIGHEST
epsilon = 1e-05
F32 = jnp.float32
BF16 = jnp.bfloat16


def split(a):
    hi = a.astype(BF16)
    lo = (a - hi.astype(F32)).astype(BF16)
    return hi, lo


def mm(a, b, dims=((1,), (0,))):
    return lax.dot_general(a, b, (dims, ((), ())), preferred_element_type=F32)


def expander(heads, width):
    head_of = lax.broadcasted_iota(jnp.int32, (heads, width), 1) // (width // heads)
    return (head_of == lax.broadcasted_iota(jnp.int32, (heads, width), 0)).astype(BF16)


def expand(a, spread):
    hi, lo = split(a)
    return mm(hi, spread) + mm(lo, spread)


def cumulative_logs(step, rate):
    span = step.shape[0]
    lower = (
        lax.broadcasted_iota(jnp.int32, (span, span), 0)
        >= lax.broadcasted_iota(jnp.int32, (span, span), 1)
    ).astype(BF16)
    logs = -step * rate
    hi = logs.astype(BF16)
    rest = logs - hi.astype(F32)
    mid, lo = split(rest)
    return mm(lower, hi) + (mm(lower, mid) + mm(lower, lo))


def state_kernel(waits, x_ref, b_ref, step_ref, rate_ref, *refs):
    out_refs, run_ref = refs[waits:-1], refs[-1]
    width = x_ref.shape[1]
    heads = step_ref.shape[1]
    spread = expander(heads, width)

    @pl.when(pl.program_id(0) == 0)
    def _():
        run_ref[...] = jnp.zeros_like(run_ref)

    step = step_ref[...]
    cum = cumulative_logs(step, rate_ref[...])
    flow = x_ref[...].astype(F32) * expand(step * jnp.exp(-cum), spread)
    flow_hi, flow_lo = split(flow)
    b = b_ref[...]
    dims = ((0,), (0,))
    added = mm(b, flow_hi, dims) + mm(b, flow_lo, dims)
    kept = expand(jnp.exp(cum[-8:]), spread)[7:8]
    run_ref[...] = (run_ref[...] + added) * kept

    @pl.when(pl.program_id(0) == pl.num_programs(0) - 1)
    def _():
        part = width // len(out_refs)
        for i, out_ref in enumerate(out_refs):
            out_ref[...] = run_ref[:, i * part : (i + 1) * part]


def inner_kernel(waits, x_ref, b_ref, c_ref, step_ref, rate_ref, skip_ref, *refs):
    y_ref, entry_ref, run_ref, log_ref = refs[waits:]
    span, width = x_ref.shape
    heads = step_ref.shape[1]
    spread = expander(heads, width)

    @pl.when(pl.program_id(0) == 0)
    def _():
        run_ref[...] = jnp.zeros_like(run_ref)
        log_ref[...] = jnp.zeros_like(log_ref)

    step = step_ref[...]
    cum = cumulative_logs(step, rate_ref[...])
    values = x_ref[...].astype(F32)
    flow_hi, flow_lo = split(values * expand(step * jnp.exp(-cum), spread))
    b = b_ref[...]
    c = c_ref[...]
    scores = mm(c, b, ((1,), (1,)))
    row = lax.broadcasted_iota(jnp.int32, (span, span), 0)
    col = lax.broadcasted_iota(jnp.int32, (span, span), 1)
    score_hi, score_lo = split(jnp.where(row >= col, scores, 0.0))
    run_hi, run_lo = split(run_ref[...])
    total = mm(score_hi, flow_hi) + mm(score_lo, flow_hi) + mm(score_hi, flow_lo)
    total = total + mm(c, run_hi) + mm(c, run_lo)
    y_ref[...] = total * expand(jnp.exp(cum), spread) + values * skip_ref[...]
    entry_ref[...] = jnp.exp(cum + log_ref[0:1])
    log_ref[...] = log_ref[...] + cum[span - 1 : span]
    dims = ((0,), (0,))
    added = mm(b, flow_hi, dims) + mm(b, flow_lo, dims)
    kept = expand(jnp.exp(cum[-8:]), spread)[7:8]
    run_ref[...] = (run_ref[...] + added) * kept


def mix_kernel(waits, y_ref, c_ref, entry_ref, incoming_ref, gate_ref, live_ref, *refs):
    mixed_ref, power_ref = refs[waits:]
    width = y_ref.shape[1]
    heads = entry_ref.shape[1]
    spread = expander(heads, width)
    inc_hi, inc_lo = split(incoming_ref[...])
    c = c_ref[...]
    extra = mm(c, inc_hi) + mm(c, inc_lo)
    y = y_ref[...] + extra * expand(entry_ref[...], spread)
    gate = gate_ref[...].astype(F32)
    mixed = y * (gate / (1.0 + jnp.exp(-gate))) * live_ref[...]
    mixed_ref[...] = mixed
    power_ref[...] = jnp.sum(mixed * mixed, axis=1, keepdims=True)


def decode_kernel(waits, state_ref, c_ref, *refs):
    (out_ref,) = refs[waits:]
    hi, lo = split(state_ref[...])
    c = c_ref[...]
    dims = ((1,), (1,))
    out_ref[...] = mm(c, hi, dims) + mm(c, lo, dims)


def anywhere(arrays):
    return [pl.BlockSpec(memory_space=pl.ANY)] * len(arrays)


def params(*kinds):
    return pltpu.CompilerParams(
        dimension_semantics=kinds, vmem_limit_bytes=56 * 1024 * 1024
    )


def shards(
    x_in, gate_in, dt_raw, b_in, c_in, lengths, decay_rate, skip_gain, norm_gain,
    dec_states, dec_x, dec_gate, dec_dt, dec_b, dec_c, slots,
):
    prompts, length_dev, groups, width = x_in.shape
    heads = dt_raw.shape[3]
    head_dim = width // heads
    state_size = b_in.shape[3]
    count = lax.axis_size("seq")
    own = lax.axis_index("seq")
    full_width = HEADS // GROUPS * HEAD_DIM
    span = SPAN
    spans = length_dev // span
    steps, dec_rows = dec_x.shape[:2]

    where_now = own * length_dev + jnp.arange(length_dev, dtype=jnp.int32)
    live = (where_now < lengths[0]).astype(F32)

    def grouped(a):
        return jnp.swapaxes(a[0], 0, 1)

    x = grouped(x_in)
    b = grouped(b_in)
    step = jax.nn.softplus(grouped(dt_raw).astype(F32)) * live[None, :, None]
    rates = decay_rate[:, None, :]
    own_logs = -jnp.sum(step, axis=1) * decay_rate

    log_rows = jnp.pad(
        jnp.repeat(own_logs, head_dim, axis=1).reshape(-1, state_size), ((0, -groups * width // state_size % 8), (0, 0))
    )
    c_count = steps * dec_rows * groups
    packed = jnp.concatenate([dec_c.astype(F32).reshape(-1, state_size), log_rows])
    arrived = [
        lax.ppermute(packed, "seq", [(i, (i + hop) % count) for i in range(count)])
        for hop in range(1, count)
    ]
    packed = jnp.stack([packed] + arrived)
    all_logs = packed[:, c_count:].reshape(count, -1)[:, : groups * width].reshape(count, groups, width)
    all_c = packed[:, :c_count].reshape(count, steps, dec_rows, groups, state_size)

    pieces = 2
    part = width // pieces
    locals_ = []
    for g in range(groups):
        waits = locals_[-1][:1] if locals_ else arrived
        locals_.append(
            pl.pallas_call(
                partial(state_kernel, len(waits)),
                grid=(spans,),
                in_specs=[
                    pl.BlockSpec((None, span, width), lambda i, g=g: (g, i, 0)),
                    pl.BlockSpec((None, span, state_size), lambda i, g=g: (g, i, 0)),
                    pl.BlockSpec((None, span, heads), lambda i, g=g: (g, i, 0)),
                    pl.BlockSpec((None, 1, heads), lambda i, g=g: (g, 0, 0)),
                ]
                + anywhere(waits),
                out_specs=[pl.BlockSpec((state_size, part), lambda i: (0, 0))] * pieces,
                out_shape=[jax.ShapeDtypeStruct((state_size, part), F32)] * pieces,
                scratch_shapes=[pltpu.VMEM((state_size, width), F32)],
                compiler_params=params("arbitrary"),
                name=f"local_state_{g}",
            )(x, b, step, rates, *waits)
        )

    places = (own - jnp.arange(count) + count) % count

    def block_decay(low, high):
        inside = (places >= low) & (places < high)
        return jnp.exp(jnp.sum(jnp.where(inside[:, None, None], all_logs, 0.0), axis=0))

    def row_of(a, g, i):
        return a[g][None, i * part : (i + 1) * part]

    rounds = []
    bit = 1
    while bit < count:
        pairs = [
            (i, i ^ bit)
            for i in range(count)
            if not i & bit or (i | (2 * bit - 1)) != count - 1
        ]
        base = own - own % bit
        other = base ^ bit
        rounds.append(
            (bit, pairs, block_decay(base, own), block_decay(base, base + bit), block_decay(other, other + bit))
        )
        bit *= 2
    totals = [locals_[g][i] for g in range(groups) for i in range(pieces)]
    prefixes = [jnp.zeros_like(t) for t in totals]
    sent = list(totals)
    for bit, pairs, before, mine, others in rounds:
        upper = (own & bit) != 0
        sent = list(totals)
        for k in range(groups * pieces):
            g, i = divmod(k, pieces)
            got = lax.ppermute(totals[k], "seq", pairs)
            prefixes[k] = jnp.where(upper, row_of(before, g, i) * got + prefixes[k], prefixes[k])
            if 2 * bit < count:
                totals[k] = jnp.where(
                    upper,
                    row_of(mine, g, i) * got + totals[k],
                    row_of(others, g, i) * totals[k] + got,
                )
    incoming = [
        jnp.concatenate(prefixes[g * pieces : (g + 1) * pieces], axis=1) for g in range(groups)
    ]

    later = block_decay(own + 1, count)
    shares = []
    for g in range(groups):
        cs = all_c[:, :, :, g].reshape(-1, state_size)
        local = jnp.concatenate(locals_[g], axis=1)
        local = lax.optimization_barrier((local, sent[-1]))[0]
        shares.append(jnp.dot(cs, local, precision=highest) * later[g][None])
    shares = jnp.stack(shares).reshape(groups, count, steps * dec_rows, width)
    carried = shares[:, 0]
    for hop in range(1, count):
        carried = carried + lax.ppermute(
            shares[:, hop], "seq", [(i, (i - hop) % count) for i in range(count)]
        )
    carried = jnp.transpose(carried.reshape(groups, steps, dec_rows, width), (1, 2, 0, 3))

    gate = grouped(gate_in)
    c = grouped(c_in)
    skip_row = jnp.repeat(skip_gain, head_dim, axis=1)

    dec_c_rows = jnp.transpose(dec_c, (1, 2, 0, 3))
    waits = sent[:1]
    kept = pl.pallas_call(
        partial(decode_kernel, len(waits)),
        grid=(dec_rows, groups),
        in_specs=[
            pl.BlockSpec((None, None, width, state_size), lambda d, g: (d, g, 0, 0)),
            pl.BlockSpec((None, None, steps, state_size), lambda d, g: (d, g, 0, 0)),
        ]
        + anywhere(waits),
        out_specs=pl.BlockSpec((None, None, steps, width), lambda d, g: (d, g, 0, 0)),
        out_shape=jax.ShapeDtypeStruct((dec_rows, groups, steps, width), F32),
        compiler_params=params("arbitrary", "arbitrary"),
        name="decode_products",
    )(dec_states.reshape(dec_rows, groups, width, state_size), dec_c_rows, *waits)

    inner = []
    for g in range(groups):

        def of_span(last, g=g):
            return pl.BlockSpec((None, span, last), lambda i: (g, i, 0))

        def of_group(rows, last, g=g):
            return pl.BlockSpec((None, rows, last), lambda i: (g, 0, 0))

        def flat(last):
            return pl.BlockSpec((span, last), lambda i: (i, 0))

        waits = [sent[min(g + 1, len(sent) - 1)], inner[-1][1] if inner else kept]
        inner.append(
            pl.pallas_call(
                partial(inner_kernel, len(waits)),
                grid=(spans,),
                in_specs=[
                    of_span(width), of_span(state_size), of_span(state_size), of_span(heads),
                    of_group(1, heads), of_group(1, width),
                ]
                + anywhere(waits),
                out_specs=[flat(width), flat(heads)],
                out_shape=[
                    jax.ShapeDtypeStruct((length_dev, width), F32),
                    jax.ShapeDtypeStruct((length_dev, heads), F32),
                ],
                scratch_shapes=[
                    pltpu.VMEM((state_size, width), F32), pltpu.VMEM((8, heads), F32)
                ],
                compiler_params=params("arbitrary"),
                name=f"inner_{g}",
            )(x, b, c, step, rates, skip_row[:, None], *waits)
        )

    kept = jnp.transpose(kept, (2, 0, 1, 3))
    from_start = jnp.where((slots >= 0)[None, :, None, None], carried, kept)
    sdt = jax.nn.softplus(dec_dt.astype(F32))
    cum = jnp.cumsum(-sdt * decay_rate, axis=0)
    products = jnp.einsum(
        "sdgn,rdgn->srdg", dec_c.astype(F32), dec_b.astype(F32), precision=highest
    )
    order = jnp.arange(steps)
    allowed = (order[:, None] >= order[None, :])[:, :, None, None, None]
    weights = jnp.exp(jnp.where(allowed, cum[:, None] - cum[None], -jnp.inf))
    weights = weights * products[..., None] * sdt[None]
    dec_vals = dec_x.astype(F32).reshape(steps, dec_rows, groups, heads, head_dim)
    result = jnp.sum(weights[..., None] * dec_vals[None], axis=1)
    result = result + skip_gain[..., None] * dec_vals
    result = result.reshape(dec_x.shape) + from_start * jnp.repeat(
        jnp.exp(cum), head_dim, axis=3
    )
    gated = result * jax.nn.silu(dec_gate.astype(F32))
    dec_power = jnp.sum(gated * gated, axis=-1)

    mixed = None
    powers = []
    for g in range(groups):

        def of_span(last, g=g):
            return pl.BlockSpec((None, span, last), lambda i: (g, i, 0))

        y, entry = inner[g]
        waits = [inner[-1][1], sent[-1]] + ([] if mixed is None else [mixed])
        mixed, power = pl.pallas_call(
            partial(mix_kernel, len(waits)),
            grid=(spans,),
            in_specs=[
                flat(width), of_span(state_size), flat(heads),
                pl.BlockSpec((state_size, width), lambda i: (0, 0)), of_span(width), flat(1),
            ]
            + anywhere(waits),
            out_specs=[of_span(width), flat(1)],
            out_shape=[
                jax.ShapeDtypeStruct((groups, length_dev, width), F32),
                jax.ShapeDtypeStruct((length_dev, 1), F32),
            ],
            input_output_aliases={} if mixed is None else {5 + len(waits): 0},
            compiler_params=params("arbitrary"),
            name=f"mix_{g}",
        )(y, c, entry, incoming[g], gate, live[:, None], *waits)
        powers.append(power)
    power = jnp.stack(powers)

    pool = lax.axis_size("pool")
    powers = jnp.concatenate([power.reshape(-1), dec_power.reshape(-1)])
    both = powers
    for hop in range(1, pool):
        both = both + lax.ppermute(powers, "pool", [(i, (i + hop) % pool) for i in range(pool)])
    both = lax.rsqrt(both / full_width + epsilon)
    scale = both[: power.size].reshape(power.shape)
    dec_scale = both[power.size :].reshape(dec_power.shape)
    prefill_out = (mixed * scale * norm_gain[:, None]).astype(BF16)
    prefill_out = jnp.swapaxes(prefill_out, 0, 1)[None]
    decode_out = (gated * dec_scale[..., None] * norm_gain).astype(BF16)
    return (prefill_out, decode_out)


def solution(mesh):
    wide = P(None, "seq", "head", "pool")
    shared = P(None, "seq", "head", None)
    per_head = P("head", "pool")
    in_specs = (
        wide, wide, wide, shared, shared, P(), per_head, per_head, per_head,
        P("seq", "head", "pool", None, None), wide, wide, wide, shared, shared, P("seq"),
    )
    return jax.shard_map(
        shards, mesh=mesh, in_specs=in_specs, out_specs=(wide, wide), check_vma=False
    )
```
